256 devices in a mesh: span: 64 (over y, x, z_lo, core), head: 4 (over z_hi).
Axes of the slice: x: 4, y: 4, z: 8 (z_hi: 4, z_lo: 2; z = z_hi * 2 + z_lo), core: 2. Of those that a mesh axis runs over, the one named last changes fastest.
Arguments:
- decoder_states: bfloat16 [131072, 1024], P('span'), may hold values from -21 to 21
- encodings: bfloat16 [4096, 128, 1024], P('span', 'head'), may hold values from -21 to 21
- neighbor_table: int32 [2048, 2, 2], P('span'), may hold values from 0 to 63, as said below
- query_weight: bfloat16 [1024, 1024], P(None, 'head'), may hold values from -0.1875 to 0.1875
- key_weight: bfloat16 [1024, 1024], P(None, 'head'), may hold values from -0.1875 to 0.1875
- value_weight: bfloat16 [1024, 1024], P(None, 'head'), may hold values from -0.1875 to 0.1875
- out_weight: bfloat16 [1024, 1024], P('head'), may hold values from -0.1875 to 0.1875
Outputs:
- attended: bfloat16 [131072, 1024], P('span', 'head')
The draws below stay inside these ranges and needn't reach their ends.
Inputs may be any that keep to these rules, and one draw needn't show every extreme that they name: neighbor_table[c, k, 0] is the database shard and neighbor_table[c, k, 1] the slot in that shard of neighbor k of span c; in each aligned block of 32 spans (the spans of one device along `span`) every shard is named by exactly one neighbor, and every slot of every shard is named exactly once in the whole table.
All inputs are finite; a program needn't handle non-finite values.
Results may differ from the reference program's by a relative error of at most 0.012.
The reference program's roundings to bfloat16 on the way (of `keys`, `values`, `queries`, `weights` and `context`) count: a program that leaves them out, or rounds other values in their place, can miss the bound.
Values may be sent and summed in bfloat16 or wider, within the bound.
A program may use at most 128 MiB of HBM per device.

```python
import jax
import jax.numpy as jnp
from jax import lax

D = 1024
HEADS = 16
HEAD_DIM = 64
SPAN_LEN = 64
NEIGH = 2
NTOK = 128
SEQ_LEN = 2048
SPANS_SEQ = 32
TOKENS = 131072
SPANS = 2048
SHARDS = 64
SLOTS = 64
PER_SOURCE = 1


def draw_decoder_states(key, part):
    subkeys = jax.random.split(jax.random.fold_in(key, 3), 1)
    values = jnp.clip(jax.random.normal(subkeys[0], (TOKENS, D), jnp.float32), -6.0, 6.0)
    return values.astype(jnp.bfloat16)


def draw_encodings(key, part):
    subkeys = jax.random.split(jax.random.fold_in(key, 5), 1)
    shape_all = (SHARDS * SLOTS, NTOK, D)
    values = jnp.clip(jax.random.normal(subkeys[0], shape_all, jnp.float32), -6.0, 6.0)
    return values.astype(jnp.bfloat16)


def draw_neighbor_table(key, part):
    dest_keys = jax.random.split(jax.random.fold_in(key, 11), SHARDS)
    orders = jax.vmap(lambda subkey: jax.random.permutation(subkey, SLOTS))(dest_keys).astype(jnp.int32)
    shard_of = orders // PER_SOURCE
    sub_index = orders % PER_SOURCE
    source_keys = jax.random.split(jax.random.fold_in(key, 12), SHARDS)
    slot_orders = jax.vmap(lambda subkey: jax.random.permutation(subkey, SLOTS))(source_keys).astype(jnp.int32)
    destination = jnp.arange(SHARDS, dtype=jnp.int32)[:, None]
    slot_of = slot_orders[shard_of, destination * PER_SOURCE + sub_index]
    return jnp.stack([shard_of, slot_of], axis=-1).reshape(SPANS, NEIGH, 2).astype(jnp.int32)


def steps_of(rng, dims, pieces, smallest, largest):
    def one(position, parts):
        draws = jax.random.uniform(jax.random.fold_in(jax.random.fold_in(rng, 6), position), (parts,), jnp.float32, smallest / len(pieces), largest / len(pieces))
        return jnp.repeat(jnp.exp(draws), dims[position] // parts).reshape((-1,) + (1,) * (len(dims) - position - 1))

    level = one(*pieces[0])
    for cut in pieces[1:]:
        level = level * one(*cut)
    return level


def normal_values(key, dims, spread, bound, pieces=(), kind=jnp.bfloat16):
    drawn = jax.random.normal(key, dims, jnp.float32) * spread
    if len(pieces) > 0:
        drawn = steps_of(key, dims, pieces, -0.22, 0.18) * drawn
    return jnp.clip(drawn, min=-bound, max=bound).astype(kind)


def setup_inputs(seed: int = 0) -> dict:
    keys = jax.random.split(jax.random.key(seed), 8)
    decoder_states = draw_decoder_states(jax.random.fold_in(keys[7], 71), 0)
    encodings = draw_encodings(jax.random.fold_in(keys[7], 71), 0)
    neighbor_table = draw_neighbor_table(jax.random.fold_in(keys[7], 71), 0)
    query_weight = normal_values(keys[3], (D, HEADS * HEAD_DIM), D ** -0.5, 0.1875, ((1, 4),))
    key_weight = normal_values(keys[4], (D, HEADS * HEAD_DIM), D ** -0.5, 0.1875, ((1, 4),))
    value_weight = normal_values(keys[5], (D, HEADS * HEAD_DIM), D ** -0.5, 0.1875, ((1, 4),))
    out_weight = normal_values(keys[6], (HEADS * HEAD_DIM, D), (HEADS * HEAD_DIM) ** -0.5, 0.1875, ((0, 4),))
    return dict(decoder_states=decoder_states, encodings=encodings, neighbor_table=neighbor_table, query_weight=query_weight, key_weight=key_weight, value_weight=value_weight, out_weight=out_weight)


def reference(decoder_states, encodings, neighbor_table, query_weight, key_weight, value_weight, out_weight):
    group_rows = (neighbor_table[:, :, 0] * SLOTS + neighbor_table[:, :, 1]).astype(jnp.int32)
    inv_root = HEAD_DIM ** -0.5
    offset = SPAN_LEN - 1
    inner_width = HEADS * HEAD_DIM

    def one_sequence(sequence):
        states = lax.dynamic_slice_in_dim(decoder_states, sequence * SEQ_LEN, SEQ_LEN, 0)
        chosen = lax.dynamic_slice_in_dim(group_rows, sequence * SPANS_SEQ, SPANS_SEQ, 0).reshape(-1)
        flattened = encodings[chosen].reshape(-1, D)
        key_rows = jnp.dot(flattened, key_weight, preferred_element_type=jnp.float32).astype(jnp.bfloat16)
        key_rows = key_rows.reshape(SPANS_SEQ, NEIGH * NTOK, HEADS, HEAD_DIM)
        value_rows = jnp.dot(flattened, value_weight, preferred_element_type=jnp.float32).astype(jnp.bfloat16)
        value_rows = value_rows.reshape(SPANS_SEQ, NEIGH * NTOK, HEADS, HEAD_DIM)
        queries = jnp.dot(states, query_weight, preferred_element_type=jnp.float32).astype(jnp.bfloat16)
        shifted = jnp.concatenate([queries[offset:], jnp.zeros((offset, inner_width), jnp.bfloat16)], axis=0)
        shifted = shifted.reshape(SPANS_SEQ, SPAN_LEN, HEADS, HEAD_DIM)
        scores = jnp.einsum("cqhd,ckhd->chqk", shifted.astype(jnp.float32), key_rows.astype(jnp.float32)) * inv_root
        weights = jax.nn.softmax(scores, axis=-1).astype(jnp.bfloat16)
        context = jnp.einsum("chqk,ckhd->cqhd", weights.astype(jnp.float32), value_rows.astype(jnp.float32))
        context = context.astype(jnp.bfloat16).reshape(SEQ_LEN, inner_width)
        context = jnp.concatenate([jnp.zeros((offset, inner_width), jnp.bfloat16), context[:SEQ_LEN - offset]], axis=0)
        return jnp.dot(context, out_weight, preferred_element_type=jnp.float32).astype(jnp.bfloat16)

    sequences = TOKENS // SEQ_LEN
    outputs = lax.map(one_sequence, jnp.arange(sequences, dtype=jnp.int32))
    return outputs.reshape(TOKENS, D)
```

```python
import functools

import jax
import jax.numpy as jnp
from jax import lax
from jax.experimental import pallas as pl
from jax.experimental.pallas import tpu as pltpu
from jax.sharding import PartitionSpec as P

HEAD_DIM = 64
SPAN_LEN = 64
SEQ_LEN = 2048
D = 1024
HEADS = 16
SPANS = 32
OFFSET = SPAN_LEN - 1
GROUP = 256
F32 = jnp.float32
BF16 = jnp.bfloat16


def head_mask(rows, cols):
    r = lax.broadcasted_iota(jnp.int32, (rows, cols), 0) // HEAD_DIM
    c = lax.broadcasted_iota(jnp.int32, (rows, cols), 1) // HEAD_DIM
    return r == c


def attention_kernel(ids, q_ref, a_ref, b_ref, ctx_ref, lse_ref):
    mask = head_mask(GROUP, GROUP)
    ones = jnp.where(mask, 1.0, 0.0).astype(BF16)
    lane = lax.broadcasted_iota(jnp.int32, (SPAN_LEN, 128), 1)
    low = lane < HEAD_DIM
    lses = jnp.zeros((SPAN_LEN, 128), F32)
    for g in range(D // GROUP):
        cols = slice(g * GROUP, (g + 1) * GROUP)
        vcols = slice(D + g * GROUP, D + (g + 1) * GROUP)
        k4 = jnp.concatenate([a_ref[0, :, cols], b_ref[0, :, cols]], axis=0)
        v4 = jnp.concatenate([a_ref[0, :, vcols], b_ref[0, :, vcols]], axis=0)
        zero = jnp.zeros((GROUP, GROUP), BF16)
        kbd = jnp.where(mask, jnp.concatenate([k4] * 4, axis=0), zero)
        vbd = jnp.where(mask, jnp.concatenate([v4] * 4, axis=0), zero)
        s = lax.dot_general(
            q_ref[:, cols], kbd, (((1,), (1,)), ((), ())), preferred_element_type=F32
        ) * (HEAD_DIM ** -0.5)
        tops = []
        for half in range(2):
            part = s[:, half * 128 : (half + 1) * 128]
            m0 = jnp.max(jnp.where(low, part, -jnp.inf), axis=1, keepdims=True)
            m1 = jnp.max(jnp.where(low, -jnp.inf, part), axis=1, keepdims=True)
            tops.append(jnp.where(low, m0, m1))
        top = jnp.concatenate(tops, axis=1)
        p = jnp.exp(s - top).astype(BF16)
        total = jnp.dot(p, ones, preferred_element_type=F32)
        c = jnp.dot(p, vbd, preferred_element_type=F32)
        ctx_ref[:, cols] = (c / total).astype(BF16)
        lse = top + jnp.log(total)
        for n in range(4):
            lses = jnp.where(lane == g * 4 + n, lse[:, n * 64 : n * 64 + 1], lses)
    lse_ref[...] = lses[:, :HEADS]


def attention(ids, queries, projected):
    spec = pltpu.PrefetchScalarGridSpec(
        num_scalar_prefetch=1,
        grid=(SPANS,),
        in_specs=[
            pl.BlockSpec((SPAN_LEN, D), lambda j, ids: (j, 0)),
            pl.BlockSpec((1, 32, 2 * D), lambda j, ids: (ids[2 * j], 0, 0)),
            pl.BlockSpec((1, 32, 2 * D), lambda j, ids: (ids[2 * j + 1], 0, 0)),
        ],
        out_specs=[
            pl.BlockSpec((SPAN_LEN, D), lambda j, ids: (j, 0)),
            pl.BlockSpec((SPAN_LEN, HEADS), lambda j, ids: (j, 0)),
        ],
    )
    return pl.pallas_call(
        attention_kernel,
        grid_spec=spec,
        out_shape=[
            jax.ShapeDtypeStruct((SEQ_LEN, D), BF16),
            jax.ShapeDtypeStruct((SEQ_LEN, HEADS), F32),
        ],
        cost_estimate=pl.CostEstimate(
            flops=8 * SEQ_LEN * D * GROUP, bytes_accessed=16 << 20, transcendentals=1 << 21
        ),
    )(ids, queries, projected, projected)


def body(
    decoder_states, encodings, neighbor_table, query_weight, key_weight, value_weight, out_weight
):
    s = lax.axis_index("span")
    h = lax.axis_index("head")
    shard_ids = neighbor_table[:, :, 0].reshape(-1)
    slot_ids = neighbor_table[:, :, 1].reshape(-1)
    numbering = jnp.arange(64, dtype=jnp.int32)
    placed = shard_ids[None, :] == numbering[:, None]
    request = jnp.sum(jnp.where(placed, slot_ids[None, :], 0), axis=1)
    wanted = lax.all_to_all(request, "span", split_axis=0, concat_axis=0, tiled=True)

    column_pieces = [
        lax.dynamic_slice_in_dim(w, s * 16, 16, 0)
        for w in (query_weight, key_weight, value_weight)
    ]
    small = lax.all_gather(jnp.concatenate(column_pieces, axis=0), "head", axis=1, tiled=True)
    out_piece = lax.dynamic_slice_in_dim(out_weight, s * 4, 4, 0)
    out_small = lax.all_gather(out_piece, "head", axis=0, tiled=True)
    pieces = jnp.concatenate([small, out_small], axis=0)
    whole = lax.all_gather(pieces, "span", axis=0)

    selected = encodings[wanted]
    arrived = lax.all_to_all(selected, "span", split_axis=0, concat_axis=0, tiled=True)

    whole_q = whole[:, 0:16].reshape(D, D)
    whole_k = whole[:, 16:32].reshape(D, D)
    whole_v = whole[:, 32:48].reshape(D, D)
    whole_o = whole[:, 48:64].reshape(64, 4, 4, D).transpose(1, 0, 2, 3).reshape(D, D)

    shifted = jnp.concatenate(
        [decoder_states[OFFSET:], jnp.zeros((OFFSET, D), BF16)], axis=0
    )
    queries = jnp.dot(shifted, whole_q, preferred_element_type=F32).astype(BF16)
    both = jnp.concatenate([whole_k, whole_v], axis=1)
    projected = jnp.dot(
        arrived.reshape(-1, D), both, preferred_element_type=F32
    ).astype(BF16).reshape(64, 32, 2 * D)
    ctx, lse = attention(shard_ids, queries, projected)
    all_lse = lax.all_gather(lse, "head", axis=0)
    share = jnp.exp(lse - jax.nn.logsumexp(all_lse, axis=0))
    share = jnp.repeat(share, HEAD_DIM, axis=1)
    scaled = (ctx.astype(F32) * share).astype(BF16)
    partial = jnp.dot(scaled, whole_o, preferred_element_type=F32).astype(BF16)
    partial = jnp.concatenate([jnp.zeros((OFFSET, D), BF16), partial[: SEQ_LEN - OFFSET]], axis=0)
    return lax.psum_scatter(partial, "head", scatter_dimension=1, tiled=True)


def solution(mesh):
    return jax.shard_map(
        body,
        mesh=mesh,
        in_specs=(
            P("span", None),
            P("span", "head", None),
            P("span", None, None),
            P(None, "head"),
            P(None, "head"),
            P(None, "head"),
            P("head", None),
        ),
        out_specs=P("span", "head"),
        check_vma=False,
    )
```

```python
import jax
import jax.numpy as jnp
from jax import lax
from jax.experimental import pallas as pl
from jax.experimental.pallas import tpu as pltpu
from jax.sharding import PartitionSpec as P

HEAD_DIM = 64
SPAN_LEN = 64
SEQ_LEN = 2048
D = 1024
HEADS = 16
SPANS = 32
OFFSET = SPAN_LEN - 1
GROUP = 256
F32 = jnp.float32
BF16 = jnp.bfloat16


def head_mask(rows, cols):
    r = lax.broadcasted_iota(jnp.int32, (rows, cols), 0) // HEAD_DIM
    c = lax.broadcasted_iota(jnp.int32, (rows, cols), 1) // HEAD_DIM
    return r == c


MESH = pl.DeviceIdType.MESH
BLK = 128
NB = SEQ_LEN // BLK


def attention_block(b, ids, q_ref, kv_ref, ctx, lse_own):
    mask = head_mask(GROUP, GROUP)
    ones = jnp.where(mask, 1.0, 0.0).astype(BF16)
    zero = jnp.zeros((GROUP, GROUP), BF16)
    lane = lax.broadcasted_iota(jnp.int32, (SPAN_LEN, 128), 1)
    low = lane < HEAD_DIM
    stats = []
    for sp in range(BLK // SPAN_LEN):
        j = b * (BLK // SPAN_LEN) + sp
        first = ids[2 * j]
        second = ids[2 * j + 1]
        rows = pl.ds(pl.multiple_of(j * SPAN_LEN, SPAN_LEN), SPAN_LEN)
        lses = jnp.zeros((SPAN_LEN, 128), F32)
        for g in range(D // GROUP):
            cols = slice(g * GROUP, (g + 1) * GROUP)
            vcols = slice(D + g * GROUP, D + (g + 1) * GROUP)
            k4 = jnp.concatenate([kv_ref[first, :, cols], kv_ref[second, :, cols]], axis=0)
            v4 = jnp.concatenate([kv_ref[first, :, vcols], kv_ref[second, :, vcols]], axis=0)
            kbd = jnp.where(mask, jnp.concatenate([k4] * 4, axis=0), zero)
            vbd = jnp.where(mask, jnp.concatenate([v4] * 4, axis=0), zero)
            s = lax.dot_general(
                q_ref[rows, cols], kbd, (((1,), (1,)), ((), ())), preferred_element_type=F32
            ) * (HEAD_DIM ** -0.5)
            tops = []
            for half in range(2):
                part = s[:, half * 128 : (half + 1) * 128]
                m0 = jnp.max(jnp.where(low, part, -jnp.inf), axis=1, keepdims=True)
                m1 = jnp.max(jnp.where(low, -jnp.inf, part), axis=1, keepdims=True)
                tops.append(jnp.where(low, m0, m1))
            top = jnp.concatenate(tops, axis=1)
            p = jnp.exp(s - top).astype(BF16)
            total = jnp.dot(p, ones, preferred_element_type=F32)
            c = jnp.dot(p, vbd, preferred_element_type=F32)
            ctx[b, sp * SPAN_LEN : (sp + 1) * SPAN_LEN, cols] = (c / total).astype(BF16)
            lse = top + jnp.log(total)
            for n in range(4):
                lses = jnp.where(lane == g * 4 + n, lse[:, n * 64 : n * 64 + 1], lses)
        stats.append(lses)
    lse_own[b] = jnp.concatenate(stats, axis=0).T[:HEADS]


def combine_kernel(
    ids, q_ref, kv_ref, o_ref, out_ref,
    ctx, lse_own, lse_in, opp, opp_in, side, own, sendb, sum_in,
    lse_send, lse_recv, opp_send, opp_recv, sum_send, sum_recv,
):
    h = lax.axis_index("head")
    peers = [(h + d) % 4 for d in range(4)]
    toward = (peers[1], peers[3])
    barrier = pltpu.get_barrier_semaphore()
    for d in range(1, 4):
        pl.semaphore_signal(barrier, inc=1, device_id={"head": peers[d]}, device_id_type=MESH)
    pl.semaphore_wait(barrier, 3)

    def lse_copy(d, b):
        return pltpu.make_async_remote_copy(
            src_ref=lse_own.at[b], dst_ref=lse_in.at[d - 1, b],
            send_sem=lse_send.at[d - 1], recv_sem=lse_recv.at[d - 1, b],
            device_id={"head": peers[d]}, device_id_type=MESH,
        )

    def opp_copy(w, b):
        return pltpu.make_async_remote_copy(
            src_ref=opp.at[w, b], dst_ref=opp_in.at[w, b],
            send_sem=opp_send.at[w], recv_sem=opp_recv.at[w, b],
            device_id={"head": toward[w]}, device_id_type=MESH,
        )

    def sum_copy(w, b):
        return pltpu.make_async_remote_copy(
            src_ref=sendb.at[w, b], dst_ref=sum_in.at[w, b],
            send_sem=sum_send.at[w], recv_sem=sum_recv.at[w, b],
            device_id={"head": toward[w]}, device_id_type=MESH,
        )

    row = lax.broadcasted_iota(jnp.int32, (2 * HEADS, D), 0) % HEADS
    col = lax.broadcasted_iota(jnp.int32, (2 * HEADS, D), 1) // HEAD_DIM
    expand = jnp.where(row == col, 1.0, 0.0).astype(BF16)

    def finish(b):
        for w in range(2):
            sum_copy(w, b).wait_recv()
        rows = pl.ds(pl.multiple_of(b * BLK, BLK), BLK)
        total = own[b] + (sum_in[0, b].astype(F32) + sum_in[1, b].astype(F32))
        out_ref[rows, :] = total.astype(BF16)

    def forward(b):
        half = BLK // 2
        for w in range(2):
            opp_copy(w, b).wait_recv()
            part = opp_in[w, b].astype(F32)
            if w == 0:
                top, low = side[w, b, :half] + part, side[w, b, half:]
            else:
                top, low = side[w, b, :half], side[w, b, half:] + part
            sendb[w, b, :half] = top.astype(BF16)
            sendb[w, b, half:] = low.astype(BF16)
            sum_copy(w, b).start()

    def project(b):
        for d in range(1, 4):
            lse_copy(d, b).wait_recv()
        mine = lse_own[b]
        others = [lse_in[d, b] for d in range(3)]
        top = jnp.maximum(jnp.maximum(mine, others[0]), jnp.maximum(others[1], others[2]))
        part = jnp.exp(mine - top)
        total = part
        for other in others:
            total = total + jnp.exp(other - top)
        share = part / total
        high = share.astype(BF16).astype(F32)
        both = jnp.concatenate([high, share - high], axis=0).T.astype(BF16)
        wide = jnp.dot(both, expand, preferred_element_type=F32)
        scaled = (ctx[b].astype(F32) * wide).astype(BF16)
        far = jnp.dot(scaled, o_ref[peers[2]], preferred_element_type=F32).astype(BF16)
        for w in range(2):
            opp[w, b] = far[w * (BLK // 2) : (w + 1) * (BLK // 2)]
        side[0, b] = jnp.dot(scaled, o_ref[peers[1]], preferred_element_type=F32)
        for w in range(2):
            opp_copy(w, b).start()
        side[1, b] = jnp.dot(scaled, o_ref[peers[3]], preferred_element_type=F32)
        own[b] = jnp.dot(scaled, o_ref[h], preferred_element_type=F32)

    def attend(b):
        attention_block(b, ids, q_ref, kv_ref, ctx, lse_own)
        for d in range(1, 4):
            lse_copy(d, b).start()

    stages = ((finish, 6), (forward, 4), (project, 2), (attend, 0))

    def step(i, carry):
        for stage, lag in stages:
            b = i - lag

            @pl.when(jnp.logical_and(b >= 0, b < NB))
            def _():
                stage(b)

        return carry

    lax.fori_loop(0, NB + 6, step, 0)

    def drain(ref, sem):
        pltpu.make_async_copy(ref, ref, sem).wait()

    for d in range(3):
        drain(lse_own, lse_send.at[d])
    for w in range(2):
        drain(opp.at[w], opp_send.at[w])
        drain(sendb.at[w], sum_send.at[w])


def combine(ids, queries, projected, columns):
    vmem = pl.BlockSpec(memory_space=pltpu.VMEM)
    return pl.pallas_call(
        combine_kernel,
        out_shape=jax.ShapeDtypeStruct((SEQ_LEN, 256), BF16),
        in_specs=[pl.BlockSpec(memory_space=pltpu.SMEM), vmem, vmem, vmem],
        out_specs=vmem,
        scratch_shapes=[
            pltpu.VMEM((NB, BLK, D), BF16),
            pltpu.VMEM((NB, HEADS, BLK), F32),
            pltpu.VMEM((3, NB, HEADS, BLK), F32),
            pltpu.VMEM((2, NB, BLK // 2, 256), BF16),
            pltpu.VMEM((2, NB, BLK // 2, 256), BF16),
            pltpu.VMEM((2, NB, BLK, 256), F32),
            pltpu.VMEM((NB, BLK, 256), F32),
            pltpu.VMEM((2, NB, BLK, 256), BF16),
            pltpu.VMEM((2, NB, BLK, 256), BF16),
            pltpu.SemaphoreType.DMA((3,)),
            pltpu.SemaphoreType.DMA((3, NB)),
            pltpu.SemaphoreType.DMA((2,)),
            pltpu.SemaphoreType.DMA((2, NB)),
            pltpu.SemaphoreType.DMA((2,)),
            pltpu.SemaphoreType.DMA((2, NB)),
        ],
        compiler_params=pltpu.CompilerParams(
            collective_id=1, has_side_effects=True, vmem_limit_bytes=60 << 20
        ),
        cost_estimate=pl.CostEstimate(
            flops=60_000_000_000, bytes_accessed=16 << 20, transcendentals=1 << 21
        ),
        name="combine",
    )(ids, queries, projected, columns)


def body(
    decoder_states, encodings, neighbor_table, query_weight, key_weight, value_weight, out_weight
):
    s = lax.axis_index("span")
    h = lax.axis_index("head")
    shard_ids = neighbor_table[:, :, 0].reshape(-1)
    slot_ids = neighbor_table[:, :, 1].reshape(-1)
    numbering = jnp.arange(64, dtype=jnp.int32)
    placed = shard_ids[None, :] == numbering[:, None]
    request = jnp.sum(jnp.where(placed, slot_ids[None, :], 0), axis=1)
    wanted = lax.all_to_all(request, "span", split_axis=0, concat_axis=0, tiled=True)

    column_pieces = [
        lax.dynamic_slice_in_dim(w, s * 16, 16, 0)
        for w in (query_weight, key_weight, value_weight)
    ]
    small = lax.all_gather(jnp.concatenate(column_pieces, axis=0), "head", axis=1, tiled=True)
    out_piece = lax.dynamic_slice_in_dim(out_weight, s * 4, 4, 0)
    out_small = lax.all_gather(out_piece, "head", axis=0, tiled=True)
    pieces = jnp.concatenate([small, out_small], axis=0)
    whole = lax.all_gather(pieces, "span", axis=0)

    selected = encodings[wanted]
    arrived = lax.all_to_all(selected, "span", split_axis=0, concat_axis=0, tiled=True)

    whole_q = whole[:, 0:16].reshape(D, D)
    whole_k = whole[:, 16:32].reshape(D, D)
    whole_v = whole[:, 32:48].reshape(D, D)
    whole_o = whole[:, 48:64].reshape(64, 4, 4, D).transpose(1, 0, 2, 3).reshape(D, D)

    shifted = jnp.concatenate(
        [decoder_states[OFFSET:], jnp.zeros((OFFSET, D), BF16)], axis=0
    )
    queries = jnp.dot(shifted, whole_q, preferred_element_type=F32).astype(BF16)
    both = jnp.concatenate([whole_k, whole_v], axis=1)
    projected = jnp.dot(
        arrived.reshape(-1, D), both, preferred_element_type=F32
    ).astype(BF16).reshape(64, 32, 2 * D)
    columns = whole_o.reshape(D, 4, 256).transpose(1, 0, 2)
    summed = combine(shard_ids, queries, projected, columns)
    return jnp.concatenate([jnp.zeros((OFFSET, 256), BF16), summed[: SEQ_LEN - OFFSET]], axis=0)


def solution(mesh):
    return jax.shard_map(
        body,
        mesh=mesh,
        in_specs=(
            P("span", None),
            P("span", "head", None),
            P("span", None, None),
            P(None, "head"),
            P(None, "head"),
            P(None, "head"),
            P("head", None),
        ),
        out_specs=P("span", "head"),
        check_vma=False,
    )
```

```python
import functools

import jax
import jax.numpy as jnp
from jax import lax
from jax.experimental import pallas as pl
from jax.experimental.pallas import tpu as pltpu
from jax.sharding import PartitionSpec as P

HEAD_DIM = 64
SPAN_LEN = 64
SEQ_LEN = 2048
D = 1024
HEADS = 16
SPANS = 32
SHARDS = 64
NTOK_PART = 32
OFFSET = SPAN_LEN - 1
GROUP = 256
BLK = 128
NB = SEQ_LEN // BLK
QT = 256
F32 = jnp.float32
BF16 = jnp.bfloat16
MESH = pl.DeviceIdType.MESH


def far(o):
    return min(o[0], 4 - o[0]) + min(o[1], 4 - o[1]) + o[2]


OFFSETS = [(0, 0, 0, 0)] + sorted(
    [
        (oy, ox, oz, oc)
        for oy in range(4)
        for ox in range(4)
        for oz in range(2)
        for oc in range(2)
        if (oy, ox, oz, oc) != (0, 0, 0, 0)
    ],
    key=lambda o: -far(o),
)


def head_mask(rows, cols):
    r = lax.broadcasted_iota(jnp.int32, (rows, cols), 0) // HEAD_DIM
    c = lax.broadcasted_iota(jnp.int32, (rows, cols), 1) // HEAD_DIM
    return r == c


def attention_block(b, place, q, kv, ctx, lse_own):
    mask = head_mask(GROUP, GROUP)
    ones = jnp.where(mask, 1.0, 0.0).astype(BF16)
    zero = jnp.zeros((GROUP, GROUP), BF16)
    lane = lax.broadcasted_iota(jnp.int32, (SPAN_LEN, 128), 1)
    low = lane < HEAD_DIM
    stats = []
    for sp in range(BLK // SPAN_LEN):
        j = b * (BLK // SPAN_LEN) + sp
        first = place[2 * j]
        second = place[2 * j + 1]
        rows = pl.ds(pl.multiple_of(j * SPAN_LEN, SPAN_LEN), SPAN_LEN)
        lses = jnp.zeros((SPAN_LEN, 128), F32)
        for g in range(D // GROUP):
            cols = slice(g * GROUP, (g + 1) * GROUP)
            k4 = jnp.concatenate([kv[g, first], kv[g, second]], axis=0)
            v4 = jnp.concatenate([kv[4 + g, first], kv[4 + g, second]], axis=0)
            kbd = jnp.where(mask, jnp.concatenate([k4] * 4, axis=0), zero)
            vbd = jnp.where(mask, jnp.concatenate([v4] * 4, axis=0), zero)
            s = lax.dot_general(
                q[rows, cols], kbd, (((1,), (1,)), ((), ())), preferred_element_type=F32
            ) * (HEAD_DIM ** -0.5)
            tops = []
            for half in range(2):
                part = s[:, half * 128 : (half + 1) * 128]
                m0 = jnp.max(jnp.where(low, part, -jnp.inf), axis=1, keepdims=True)
                m1 = jnp.max(jnp.where(low, -jnp.inf, part), axis=1, keepdims=True)
                tops.append(jnp.where(low, m0, m1))
            top = jnp.concatenate(tops, axis=1)
            p = jnp.exp(s - top).astype(BF16)
            total = jnp.dot(p, ones, preferred_element_type=F32)
            c = jnp.dot(p, vbd, preferred_element_type=F32)
            ctx[b, sp * SPAN_LEN : (sp + 1) * SPAN_LEN, cols] = (c / total).astype(BF16)
            lse = top + jnp.log(total)
            for n in range(4):
                lses = jnp.where(lane == g * 4 + n, lse[:, n * 64 : n * 64 + 1], lses)
        stats.append(lses)
    lse_own[b] = jnp.concatenate(stats, axis=0).T[:HEADS]


def kernel(
    place, req, enc_hbm, dec_hbm, wq, wk, wv, wo, out,
    enc, dec, want, want_s, stage, arr, w, q, carry, kv,
    ctx, lse_own, lse_in, opp, opp_in, side, own, sendb, sum_in,
    load_sem, req_send, req_recv, arr_send, arr_recv,
    z_send, z_recv, a_send, a_recv, one_send, one_recv, two_send, two_recv, c_send, c_recv,
    lse_send, lse_recv, opp_send, opp_recv, sum_send, sum_recv,
):
    h = lax.axis_index("head")
    s = lax.axis_index("span")
    core = s % 2
    zl = (s // 2) % 2
    x = (s // 4) % 4
    y = s // 16
    peers = [(h + d) % 4 for d in range(4)]
    toward = (peers[1], peers[3])

    def index(yy, xx, zz, cc):
        return ((yy * 4 + xx) * 2 + zz) * 2 + cc

    def target(o):
        return index((y + o[0]) % 4, (x + o[1]) % 4, (zl + o[2]) % 2, (core + o[3]) % 2)

    def send(src, dst, send_sem, recv_sem, to):
        return pltpu.make_async_remote_copy(
            src_ref=src, dst_ref=dst, send_sem=send_sem, recv_sem=recv_sem,
            device_id=to, device_id_type=MESH,
        )

    loads = [
        pltpu.make_async_copy(src, w.at[h, i], load_sem.at[i])
        for i, src in enumerate((wq, wk, wv))
    ] + [
        pltpu.make_async_copy(
            wo.at[:, :, :, k * 256 : (k + 1) * 256],
            w.at[h, 3, k // 2, 2 * (k % 2) : 2 * (k % 2) + 2],
            load_sem.at[3 + k],
        )
        for k in range(4)
    ]
    enc_load = pltpu.make_async_copy(enc_hbm, enc, load_sem.at[7])
    dec_load = pltpu.make_async_copy(dec_hbm, dec.at[pl.ds(0, SEQ_LEN)], load_sem.at[8])
    for load in loads:
        load.start()
    enc_load.start()
    dec_load.start()

    barrier = pltpu.get_barrier_semaphore()
    for o in OFFSETS[1:]:
        pl.semaphore_signal(barrier, inc=1, device_id={"span": target(o)}, device_id_type=MESH)
    for d in range(1, 4):
        pl.semaphore_signal(barrier, inc=1, device_id={"head": peers[d]}, device_id_type=MESH)
    want[s] = req[s]
    dec[SEQ_LEN:] = jnp.zeros((SPAN_LEN, D), BF16)
    pl.semaphore_wait(barrier, SHARDS - 1 + 3)

    for o in OFFSETS[1:]:
        t = target(o)
        send(req.at[t], want.at[s], req_send, req_recv, {"span": t}).start()

    def z_copy(d):
        piece = w.at[h, :, core, y, x, pl.ds(pl.multiple_of(zl * 16, 16), 16), :]
        return send(piece, piece, z_send.at[d - 1], z_recv.at[d - 1], {"head": peers[d]})

    def a_copy(d):
        piece = w.at[peers[d], :, core, y, x, pl.ds(pl.multiple_of(zl * 16, 16), 16), :]
        to = {"span": index(y, x, 1 - zl, core)}
        return send(piece, piece, a_send.at[d - 1], a_recv.at[d - 1], to)

    def one_copy(half, e, d):
        piece = w.at[peers[d], 2 * half : 2 * half + 2, core, y, x]
        to = index(y, (x + e) % 4, zl, core) if half == 0 else index((y + e) % 4, x, zl, core)
        n = (half * 3 + e - 1) * 3 + d - 1
        return send(piece, piece, one_send.at[n], one_recv.at[n], {"span": to})

    def two_copy(half, e, d):
        if half == 0:
            piece = w.at[peers[d], 0:2, core, y]
            to = index((y + e) % 4, x, zl, core)
        else:
            piece = w.at[peers[d], 2:4, core, :, x]
            to = index(y, (x + e) % 4, zl, core)
        n = (half * 3 + e - 1) * 3 + d - 1
        return send(piece, piece, two_send.at[n], two_recv.at[n], {"span": to})

    def c_copy(d):
        piece = w.at[peers[d], :, core]
        return send(piece, piece, c_send.at[d - 1], c_recv.at[d - 1], {"span": index(y, x, zl, 1 - core)})

    ring = [(half, e, d) for e in (1, 2, 3) for d in (1, 2, 3) for half in (0, 1)]
    weight_copies = [z_copy(d) for d in (1, 2, 3)] + [a_copy(d) for d in (1, 2, 3)]
    weight_copies += [one_copy(*r) for r in ring] + [two_copy(*r) for r in ring]
    weight_copies += [c_copy(d) for d in (1, 2, 3)]

    def arr_copy(i):
        to = {"span": target(OFFSETS[i])}
        return send(stage.at[i], arr.at[i], arr_send, arr_recv.at[i], to)

    def issue(lo, hi):
        for i in range(lo, hi):
            stage[i] = enc[want_s[target(OFFSETS[i]), 0, 0]]
            if i > 1:
                arr_copy(i - 1).start()

    for load in loads:
        load.wait()
    for d in (1, 2, 3):
        z_copy(d).start()
    everyone = pltpu.make_async_copy(
        want.at[pl.ds(0, SHARDS - 1)], want.at[pl.ds(0, SHARDS - 1)], req_recv
    )
    everyone.wait()
    to_scalar = pltpu.make_async_copy(want, want_s, load_sem.at[9])
    to_scalar.start()
    enc_load.wait()
    to_scalar.wait()
    issue(1, 5)
    for d in (1, 2, 3):
        z_copy(d).wait_recv()
    for d in (1, 2, 3):
        a_copy(d).start()
    issue(5, 9)
    for d in (1, 2, 3):
        a_copy(d).wait_recv()
    for r in ring:
        one_copy(*r).start()
    issue(9, 17)
    for r in ring:
        one_copy(*r).wait_recv()
    for r in ring:
        two_copy(*r).start()
    issue(17, SHARDS)
    arr[0] = enc[want_s[s, 0, 0]]
    arr_copy(SHARDS - 1).start()
    for r in ring:
        two_copy(*r).wait_recv()
    for d in (1, 2, 3):
        c_copy(d).start()
    dec_load.wait()
    for d in (1, 2, 3):
        c_copy(d).wait_recv()

    def weight(group, i):
        return w[group, i].reshape(D, GROUP)

    for g in range(4):
        head_rows = jnp.dot(dec[48:64], weight(g, 0), preferred_element_type=F32)
        carry[:, g * GROUP : (g + 1) * GROUP] = head_rows[8:16]

    first_row = lax.broadcasted_iota(jnp.int32, (QT, GROUP), 0) == 0

    def query_tile(t, state):
        source = dec[pl.ds(pl.multiple_of(t * QT + 64, 64), QT)]
        for g in range(4):
            cols = slice(g * GROUP, (g + 1) * GROUP)
            tile = jnp.dot(source, weight(g, 0), preferred_element_type=F32)
            before = carry[7:8, cols]
            moved = jnp.where(first_row, before, pltpu.roll(tile, 1, 0))
            q[pl.ds(pl.multiple_of(t * QT, QT), QT), cols] = moved.astype(BF16)
            carry[:, cols] = tile[QT - 8 :]
        return state

    lax.fori_loop(0, SEQ_LEN // QT, query_tile, 0)

    def project_chunk(k, state):
        for i in range(8):
            n = 8 * k + i

            @pl.when(n > 0)
            def _():
                send(stage.at[n], arr.at[n], arr_send, arr_recv.at[n], {"span": s}).wait_recv()

        tokens = arr[pl.ds(8 * k, 8)].reshape(8 * NTOK_PART, D)

        def columns(n, inner):
            part = jnp.dot(tokens, weight(n % 4, 1 + n // 4), preferred_element_type=F32)
            kv[n, pl.ds(8 * k, 8)] = part.astype(BF16).reshape(8, NTOK_PART, GROUP)
            return inner

        return lax.fori_loop(0, 8, columns, state)

    lax.fori_loop(0, SHARDS // 8, project_chunk, 0)

    def lse_copy(d, b):
        return send(
            lse_own.at[b], lse_in.at[d - 1, b], lse_send.at[d - 1], lse_recv.at[d - 1, b],
            {"head": peers[d]},
        )

    def opp_copy(way, b):
        return send(
            opp.at[way, b], opp_in.at[way, b], opp_send.at[way], opp_recv.at[way, b],
            {"head": toward[way]},
        )

    def sum_copy(way, b):
        return send(
            sendb.at[way, b], sum_in.at[way, b], sum_send.at[way], sum_recv.at[way, b],
            {"head": toward[way]},
        )

    row = lax.broadcasted_iota(jnp.int32, (2 * HEADS, D), 0) % HEADS
    col = lax.broadcasted_iota(jnp.int32, (2 * HEADS, D), 1) // HEAD_DIM
    expand = jnp.where(row == col, 1.0, 0.0).astype(BF16)

    def finish(b):
        for way in range(2):
            sum_copy(way, b).wait_recv()
        rows = pl.ds(pl.multiple_of(b * BLK, BLK), BLK)
        total = own[b] + (sum_in[0, b].astype(F32) + sum_in[1, b].astype(F32))
        out[rows, :] = total.astype(BF16)

    def forward(b):
        half = BLK // 2
        for way in range(2):
            opp_copy(way, b).wait_recv()
            part = opp_in[way, b].astype(F32)
            if way == 0:
                upper, lower = side[way, b, :half] + part, side[way, b, half:]
            else:
                upper, lower = side[way, b, :half], side[way, b, half:] + part
            sendb[way, b, :half] = upper.astype(BF16)
            sendb[way, b, half:] = lower.astype(BF16)
            sum_copy(way, b).start()

    def project(b):
        for d in range(1, 4):
            lse_copy(d, b).wait_recv()
        mine = lse_own[b]
        others = [lse_in[d, b] for d in range(3)]
        top = jnp.maximum(jnp.maximum(mine, others[0]), jnp.maximum(others[1], others[2]))
        part = jnp.exp(mine - top)
        total = part
        for other in others:
            total = total + jnp.exp(other - top)
        share = part / total
        high = share.astype(BF16).astype(F32)
        both = jnp.concatenate([high, share - high], axis=0).T.astype(BF16)
        wide = jnp.dot(both, expand, preferred_element_type=F32)
        scaled = (ctx[b].astype(F32) * wide).astype(BF16)

        def columns(k):
            total = None
            for g in range(4):
                block = w[g, 3, k // 2, pl.ds(2 * (k % 2), 2)].reshape(GROUP, GROUP)
                part = jnp.dot(
                    scaled[:, g * GROUP : (g + 1) * GROUP], block, preferred_element_type=F32
                )
                total = part if total is None else total + part
            return total

        away = columns(peers[2]).astype(BF16)
        for way in range(2):
            opp[way, b] = away[way * (BLK // 2) : (way + 1) * (BLK // 2)]
        side[0, b] = columns(peers[1])
        for way in range(2):
            opp_copy(way, b).start()
        side[1, b] = columns(peers[3])
        own[b] = columns(h)

    def attend(b):
        attention_block(b, place, q, kv, ctx, lse_own)
        for d in range(1, 4):
            lse_copy(d, b).start()

    stages = ((finish, 6), (forward, 4), (project, 2), (attend, 0))

    def step(i, state):
        for work, lag in stages:
            b = i - lag

            @pl.when(jnp.logical_and(b >= 0, b < NB))
            def _():
                work(b)

        return state

    lax.fori_loop(0, NB + 6, step, 0)

    def drain(ref, sem):
        pltpu.make_async_copy(ref, ref, sem).wait()

    drain(want.at[pl.ds(0, SHARDS - 1)], req_send)
    drain(stage.at[pl.ds(0, SHARDS - 1)], arr_send)
    for copy in weight_copies:
        copy.wait_send()
    for d in range(3):
        drain(lse_own, lse_send.at[d])
    for way in range(2):
        drain(opp.at[way], opp_send.at[way])
        drain(sendb.at[way], sum_send.at[way])


def whole(place, req, encodings, decoder_states, wq, wk, wv, wo):
    vmem = pl.BlockSpec(memory_space=pltpu.VMEM)
    hbm = pl.BlockSpec(memory_space=pl.ANY)
    dma = pltpu.SemaphoreType.DMA
    return pl.pallas_call(
        kernel,
        out_shape=jax.ShapeDtypeStruct((SEQ_LEN, 256), BF16),
        in_specs=[pl.BlockSpec(memory_space=pltpu.SMEM), vmem] + [hbm] * 6,
        out_specs=vmem,
        scratch_shapes=[
            pltpu.VMEM((SHARDS, NTOK_PART, D), BF16),
            pltpu.VMEM((SEQ_LEN + SPAN_LEN, D), BF16),
            pltpu.VMEM((SHARDS, 1, 128), jnp.int32),
            pltpu.SMEM((SHARDS, 1, 128), jnp.int32),
            pltpu.VMEM((SHARDS, NTOK_PART, D), BF16),
            pltpu.VMEM((SHARDS, NTOK_PART, D), BF16),
            pltpu.VMEM((4, 4, 2, 4, 4, 32, 256), BF16),
            pltpu.VMEM((SEQ_LEN, D), BF16),
            pltpu.VMEM((8, D), F32),
            pltpu.VMEM((8, SHARDS, NTOK_PART, GROUP), BF16),
            pltpu.VMEM((NB, BLK, D), BF16),
            pltpu.VMEM((NB, HEADS, BLK), F32),
            pltpu.VMEM((3, NB, HEADS, BLK), F32),
            pltpu.VMEM((2, NB, BLK // 2, 256), BF16),
            pltpu.VMEM((2, NB, BLK // 2, 256), BF16),
            pltpu.VMEM((2, NB, BLK, 256), F32),
            pltpu.VMEM((NB, BLK, 256), F32),
            pltpu.VMEM((2, NB, BLK, 256), BF16),
            pltpu.VMEM((2, NB, BLK, 256), BF16),
            dma((10,)), dma, dma, dma, dma((SHARDS,)),
            dma((3,)), dma((3,)), dma((3,)), dma((3,)),
            dma((18,)), dma((18,)), dma((18,)), dma((18,)), dma((3,)), dma((3,)),
            dma((3,)), dma((3, NB)), dma((2,)), dma((2, NB)), dma((2,)), dma((2, NB)),
        ],
        compiler_params=pltpu.CompilerParams(
            collective_id=1, has_side_effects=True, vmem_limit_bytes=63 << 20
        ),
        cost_estimate=pl.CostEstimate(
            flops=90_000_000_000, bytes_accessed=16 << 20, transcendentals=1 << 21
        ),
        name="whole",
    )(place, req, encodings, decoder_states, wq, wk, wv, wo)


def body(
    decoder_states, encodings, neighbor_table, query_weight, key_weight, value_weight, out_weight
):
    s = lax.axis_index("span")
    shard_ids = neighbor_table[:, :, 0].reshape(-1)
    slot_ids = neighbor_table[:, :, 1].reshape(-1)
    numbering = jnp.arange(SHARDS, dtype=jnp.int32)
    placed = shard_ids[None, :] == numbering[:, None]
    request = jnp.sum(jnp.where(placed, slot_ids[None, :], 0), axis=1)
    req = jnp.broadcast_to(request[:, None, None], (SHARDS, 1, 128))

    def digits(v):
        return v // 16, (v // 4) % 4, (v // 2) % 2, v % 2

    mine, theirs = digits(s), digits(shard_ids)
    oy, ox, oz, oc = ((a - b + m) % m for a, b, m in zip(mine, theirs, (4, 4, 2, 2)))
    code = ((oy * 4 + ox) * 2 + oz) * 2 + oc
    codes = jnp.array([((o[0] * 4 + o[1]) * 2 + o[2]) * 2 + o[3] for o in OFFSETS], jnp.int32)
    place = jnp.sum(jnp.where(code[:, None] == codes[None, :], numbering[None, :], 0), axis=1)

    sliced = (2, 4, 4, 32, 256)
    summed = whole(
        place, req, encodings, decoder_states,
        query_weight.reshape(sliced), key_weight.reshape(sliced), value_weight.reshape(sliced),
        out_weight.reshape(2, 4, 32, D),
    )
    return jnp.concatenate([jnp.zeros((OFFSET, 256), BF16), summed[: SEQ_LEN - OFFSET]], axis=0)


def solution(mesh):
    return jax.shard_map(
        body,
        mesh=mesh,
        in_specs=(
            P("span", None),
            P("span", "head", None),
            P("span", None, None),
            P(None, "head"),
            P(None, "head"),
            P(None, "head"),
            P("head", None),
        ),
        out_specs=P("span", "head"),
        check_vma=False,
    )
```

```python
import functools

import jax
import jax.numpy as jnp
from jax import lax
from jax.experimental import pallas as pl
from jax.experimental.pallas import tpu as pltpu
from jax.sharding import PartitionSpec as P

HEAD_DIM = 64
SPAN_LEN = 64
SEQ_LEN = 2048
D = 1024
HEADS = 16
SPANS = 32
SHARDS = 64
NTOK_PART = 32
GROUP = 256
BLK = 128
NB = SEQ_LEN // BLK
QT = 256
F32 = jnp.float32
BF16 = jnp.bfloat16
MESH = pl.DeviceIdType.MESH


def links(o):
    ways = ((0, 0), (1, 0), (1, 1), (0, 1))
    return [*ways[o[1]], *ways[o[0]], o[2]]


def balanced(offsets):
    left, done, order = list(offsets), [0] * 5, []
    while left:

        def cost(o):
            after = [a + b for a, b in zip(done, links(o))]
            mean = sum(after) / 5
            return sum((v - mean) ** 2 for v in after) - sum(links(o))

        best = min(left, key=cost)
        left.remove(best)
        order.append(best)
        done = [a + b for a, b in zip(done, links(best))]
    return order


ALL = [(oy, ox, oz, oc) for oy in range(4) for ox in range(4) for oz in range(2) for oc in range(2)]
OFFSETS = ALL[:1] + balanced(ALL[1:])


def head_mask(rows, cols):
    r = lax.broadcasted_iota(jnp.int32, (rows, cols), 0) // HEAD_DIM
    c = lax.broadcasted_iota(jnp.int32, (rows, cols), 1) // HEAD_DIM
    return r == c


def attention_block(b, place, q, kv, ctx, lse_own):
    mask = head_mask(GROUP, GROUP)
    ones = jnp.where(mask, 1.0, 0.0).astype(BF16)
    zero = jnp.zeros((GROUP, GROUP), BF16)
    lane = lax.broadcasted_iota(jnp.int32, (SPAN_LEN, 128), 1)
    low = lane < HEAD_DIM
    stats = []
    for sp in range(BLK // SPAN_LEN):
        j = b * (BLK // SPAN_LEN) + sp
        first = place(2 * j)
        second = place(2 * j + 1)
        rows = pl.ds(pl.multiple_of(j * SPAN_LEN, SPAN_LEN), SPAN_LEN)
        lses = jnp.zeros((SPAN_LEN, 128), F32)
        for g in range(D // GROUP):
            cols = slice(g * GROUP, (g + 1) * GROUP)
            k4 = jnp.concatenate([kv[g, first], kv[g, second]], axis=0)
            v4 = jnp.concatenate([kv[4 + g, first], kv[4 + g, second]], axis=0)
            kbd = jnp.where(mask, jnp.concatenate([k4] * 4, axis=0), zero)
            vbd = jnp.where(mask, jnp.concatenate([v4] * 4, axis=0), zero)
            s = lax.dot_general(
                q[rows, cols], kbd, (((1,), (1,)), ((), ())), preferred_element_type=F32
            ) * (HEAD_DIM ** -0.5)
            tops = []
            for half in range(2):
                part = s[:, half * 128 : (half + 1) * 128]
                m0 = jnp.max(jnp.where(low, part, -jnp.inf), axis=1, keepdims=True)
                m1 = jnp.max(jnp.where(low, -jnp.inf, part), axis=1, keepdims=True)
                tops.append(jnp.where(low, m0, m1))
            top = jnp.concatenate(tops, axis=1)
            p = jnp.exp(s - top).astype(BF16)
            total = jnp.dot(p, ones, preferred_element_type=F32)
            c = jnp.dot(p, vbd, preferred_element_type=F32)
            ctx[b, sp * SPAN_LEN : (sp + 1) * SPAN_LEN, cols] = (c / total).astype(BF16)
            lse = top + jnp.log(total)
            for n in range(4):
                lses = jnp.where(lane == g * 4 + n, lse[:, n * 64 : n * 64 + 1], lses)
        stats.append(lses)
    lse_own[b] = jnp.concatenate(stats, axis=0).T[:HEADS]


def kernel(
    table, position, enc_hbm, dec_hbm, wq, wk, wv, wo, out,
    enc, dec, req, want, want_s, stage, arr, w, q, carry, kv,
    ctx, lse_own, lse_in, opp, opp_in, side, own, sendb, sum_in,
    load_sem, req_send, req_recv, arr_send, arr_recv,
    z_send, z_recv, a_send, a_recv, one_send, one_recv, two_send, two_recv, c_send, c_recv,
    lse_send, lse_recv, opp_send, opp_recv, sum_send, sum_recv,
):
    h = lax.axis_index("head")
    s = lax.axis_index("span")
    core = s % 2
    zl = (s // 2) % 2
    x = (s // 4) % 4
    y = s // 16
    peers = [(h + d) % 4 for d in range(4)]
    toward = (peers[1], peers[3])

    def index(yy, xx, zz, cc):
        return ((yy * 4 + xx) * 2 + zz) * 2 + cc

    def target(o):
        return index((y + o[0]) % 4, (x + o[1]) % 4, (zl + o[2]) % 2, (core + o[3]) % 2)

    def send(src, dst, send_sem, recv_sem, to):
        return pltpu.make_async_remote_copy(
            src_ref=src, dst_ref=dst, send_sem=send_sem, recv_sem=recv_sem,
            device_id=to, device_id_type=MESH,
        )

    loads = [
        pltpu.make_async_copy(src, w.at[h, i], load_sem.at[i])
        for i, src in ((0, wk), (1, wq), (2, wv))
    ] + [
        pltpu.make_async_copy(
            wo.at[:, :, :, k * 256 : (k + 1) * 256],
            w.at[h, 3, k // 2, 2 * (k % 2) : 2 * (k % 2) + 2],
            load_sem.at[3 + k],
        )
        for k in range(4)
    ]
    enc_load = pltpu.make_async_copy(enc_hbm, enc, load_sem.at[7])
    dec_load = pltpu.make_async_copy(dec_hbm, dec.at[pl.ds(0, SEQ_LEN)], load_sem.at[8])
    for load in loads:
        load.start()
    enc_load.start()
    dec_load.start()

    barrier = pltpu.get_barrier_semaphore()
    for o in OFFSETS[1:]:
        pl.semaphore_signal(barrier, inc=1, device_id={"span": target(o)}, device_id_type=MESH)
    for d in range(1, 4):
        pl.semaphore_signal(barrier, inc=1, device_id={"head": peers[d]}, device_id_type=MESH)
    shard_row = lax.broadcasted_iota(jnp.int32, (SHARDS, 128), 0)
    slots = jnp.zeros((SHARDS, 128), jnp.int32)
    for e in range(SHARDS):
        slots = jnp.where(shard_row == table[2 * e], table[2 * e + 1], slots)
    req[...] = slots.reshape(SHARDS, 1, 128)
    want[s] = req[s]
    dec[SEQ_LEN:] = jnp.zeros((SPAN_LEN, D), BF16)
    pl.semaphore_wait(barrier, SHARDS - 1 + 3)

    for o in OFFSETS[1:]:
        t = target(o)
        send(req.at[t], want.at[s], req_send, req_recv, {"span": t}).start()

    def z_copy(d):
        piece = w.at[h, :, core, y, x, pl.ds(pl.multiple_of(zl * 16, 16), 16), :]
        return send(piece, piece, z_send, z_recv.at[d - 1], {"head": peers[d]})

    def a_copy(d):
        piece = w.at[peers[d], :, core, y, x, pl.ds(pl.multiple_of(zl * 16, 16), 16), :]
        to = {"span": index(y, x, 1 - zl, core)}
        return send(piece, piece, a_send, a_recv.at[d - 1], to)

    def one_copy(half, e, d):
        piece = w.at[peers[d], 2 * half : 2 * half + 2, core, y, x]
        to = index(y, (x + e) % 4, zl, core) if half == 0 else index((y + e) % 4, x, zl, core)
        n = (half * 3 + e - 1) * 3 + d - 1
        return send(piece, piece, one_send, one_recv.at[n], {"span": to})

    def two_copy(group, half, e, d):
        if half == 0:
            piece = w.at[peers[d], group, core, y]
            to = index((y + e) % 4, x, zl, core)
        else:
            piece = w.at[peers[d], 2 + group, core, :, x]
            to = index(y, (x + e) % 4, zl, core)
        n = ((group * 2 + half) * 3 + e - 1) * 3 + d - 1
        return send(piece, piece, two_send.at[group], two_recv.at[n], {"span": to})

    def c_copy(group, half, d):
        piece = w.at[peers[d], 2 * half + group, core]
        n = (group * 2 + half) * 3 + d - 1
        to = {"span": index(y, x, zl, 1 - core)}
        return send(piece, piece, c_send.at[group], c_recv.at[n], to)

    ring = [(half, e, d) for e in (1, 2, 3) for d in (1, 2, 3) for half in (0, 1)]
    swap = [(half, d) for d in (1, 2, 3) for half in (0, 1)]
    def arr_copy(i):
        to = {"span": target(OFFSETS[i])}
        return send(stage.at[i], arr.at[i], arr_send, arr_recv.at[i], to)

    def issue(lo, hi):
        for i in range(lo, hi):
            stage[i] = enc[want_s[target(OFFSETS[i]), 0, 0]]
            if i > 1:
                arr_copy(i - 1).start()

    for load in loads:
        load.wait()
    for d in (1, 2, 3):
        z_copy(d).start()
    everyone = pltpu.make_async_copy(
        want.at[pl.ds(0, SHARDS - 1)], want.at[pl.ds(0, SHARDS - 1)], req_recv
    )
    everyone.wait()
    to_scalar = pltpu.make_async_copy(want, want_s, load_sem.at[9])
    to_scalar.start()
    enc_load.wait()
    to_scalar.wait()
    issue(1, 5)
    for d in (1, 2, 3):
        z_copy(d).wait_recv()
    for d in (1, 2, 3):
        a_copy(d).start()
    issue(5, 9)
    for d in (1, 2, 3):
        a_copy(d).wait_recv()
    for r in ring:
        one_copy(*r).start()
    issue(9, 13)
    for r in ring:
        one_copy(*r).wait_recv()
    for r in ring:
        two_copy(0, *r).start()
    issue(13, 21)
    for r in ring:
        two_copy(0, *r).wait_recv()
    for r in swap:
        c_copy(0, *r).start()
    issue(21, 37)
    for r in ring:
        two_copy(1, *r).start()
    issue(37, SHARDS)
    arr[0] = enc[want_s[s, 0, 0]]
    arr_copy(SHARDS - 1).start()
    for r in swap:
        c_copy(0, *r).wait_recv()

    def weight(group, i):
        return w[group, i].reshape(D, GROUP)

    def project_chunk(k, state):
        for i in range(8):
            n = 8 * k + i

            @pl.when(n > 0)
            def _():
                send(stage.at[n], arr.at[n], arr_send, arr_recv.at[n], {"span": s}).wait_recv()

        tokens = arr[pl.ds(8 * k, 8)].reshape(8 * NTOK_PART, D)

        def columns(n, inner):
            part = jnp.dot(tokens, weight(n % 4, 2 * (n // 4)), preferred_element_type=F32)
            kv[n, pl.ds(8 * k, 8)] = part.astype(BF16).reshape(8, NTOK_PART, GROUP)
            return inner

        return lax.fori_loop(0, 8, columns, state)

    lax.fori_loop(0, 4, project_chunk, 0)
    for r in ring:
        two_copy(1, *r).wait_recv()
    for r in swap:
        c_copy(1, *r).start()
    lax.fori_loop(4, 6, project_chunk, 0)
    dec_load.wait()
    for r in swap:
        c_copy(1, *r).wait_recv()

    for g in range(4):
        head_rows = jnp.dot(dec[48:64], weight(g, 1), preferred_element_type=F32)
        carry[:, g * GROUP : (g + 1) * GROUP] = head_rows[8:16]

    first_row = lax.broadcasted_iota(jnp.int32, (QT, GROUP), 0) == 0

    def query_tile(t, state):
        source = dec[pl.ds(pl.multiple_of(t * QT + 64, 64), QT)]
        for g in range(4):
            cols = slice(g * GROUP, (g + 1) * GROUP)
            tile = jnp.dot(source, weight(g, 1), preferred_element_type=F32)
            before = carry[7:8, cols]
            moved = jnp.where(first_row, before, pltpu.roll(tile, 1, 0))
            q[pl.ds(pl.multiple_of(t * QT, QT), QT), cols] = moved.astype(BF16)
            carry[:, cols] = tile[QT - 8 :]
        return state

    lax.fori_loop(0, SEQ_LEN // QT, query_tile, 0)

    lax.fori_loop(6, SHARDS // 8, project_chunk, 0)

    def lse_copy(d, b):
        return send(
            lse_own.at[b], lse_in.at[d - 1, b], lse_send.at[d - 1], lse_recv.at[d - 1, b],
            {"head": peers[d]},
        )

    def opp_copy(way, b):
        return send(
            opp.at[way, b], opp_in.at[way, b], opp_send.at[way], opp_recv.at[way, b],
            {"head": toward[way]},
        )

    def sum_copy(way, b):
        return send(
            sendb.at[way, b], sum_in.at[way, b], sum_send.at[way], sum_recv.at[way, b],
            {"head": toward[way]},
        )

    row = lax.broadcasted_iota(jnp.int32, (2 * HEADS, D), 0) % HEADS
    col = lax.broadcasted_iota(jnp.int32, (2 * HEADS, D), 1) // HEAD_DIM
    expand = jnp.where(row == col, 1.0, 0.0).astype(BF16)

    def finish(b):
        for way in range(2):
            sum_copy(way, b).wait_recv()
        total = own[b] + (sum_in[0, b].astype(F32) + sum_in[1, b].astype(F32))
        own[b] = total

        @pl.when(b == 0)
        def _():
            last = lax.broadcasted_iota(jnp.int32, (SPAN_LEN, 256), 0) == SPAN_LEN - 1
            out[:SPAN_LEN] = jnp.where(last, total[0:1], 0.0).astype(BF16)

        @pl.when(b > 0)
        def _():
            last = lax.broadcasted_iota(jnp.int32, (BLK, 256), 0) == BLK - 1
            moved = jnp.where(last, total[0:1], pltpu.roll(own[b - 1], BLK - 1, 0))
            out[pl.ds(pl.multiple_of((b - 1) * BLK + SPAN_LEN, SPAN_LEN), BLK)] = moved.astype(BF16)

        @pl.when(b == NB - 1)
        def _():
            out[SEQ_LEN - SPAN_LEN :] = pltpu.roll(total, BLK - 1, 0)[:SPAN_LEN].astype(BF16)

    def forward(b):
        half = BLK // 2
        for way in range(2):
            opp_copy(way, b).wait_recv()
            part = opp_in[way, b].astype(F32)
            if way == 0:
                upper, lower = side[way, b, :half] + part, side[way, b, half:]
            else:
                upper, lower = side[way, b, :half], side[way, b, half:] + part
            sendb[way, b, :half] = upper.astype(BF16)
            sendb[way, b, half:] = lower.astype(BF16)
            sum_copy(way, b).start()

    def project(b):
        for d in range(1, 4):
            lse_copy(d, b).wait_recv()
        mine = lse_own[b]
        others = [lse_in[d, b] for d in range(3)]
        top = jnp.maximum(jnp.maximum(mine, others[0]), jnp.maximum(others[1], others[2]))
        part = jnp.exp(mine - top)
        total = part
        for other in others:
            total = total + jnp.exp(other - top)
        share = part / total
        high = share.astype(BF16).astype(F32)
        both = jnp.concatenate([high, share - high], axis=0).T.astype(BF16)
        wide = jnp.dot(both, expand, preferred_element_type=F32)
        scaled = (ctx[b].astype(F32) * wide).astype(BF16)

        def columns(k):
            total = None
            for g in range(4):
                block = w[g, 3, k // 2, pl.ds(2 * (k % 2), 2)].reshape(GROUP, GROUP)
                part = jnp.dot(
                    scaled[:, g * GROUP : (g + 1) * GROUP], block, preferred_element_type=F32
                )
                total = part if total is None else total + part
            return total

        away = columns(peers[2]).astype(BF16)
        for way in range(2):
            opp[way, b] = away[way * (BLK // 2) : (way + 1) * (BLK // 2)]
        side[0, b] = columns(peers[1])
        for way in range(2):
            opp_copy(way, b).start()
        side[1, b] = columns(peers[3])
        own[b] = columns(h)

    def place(e):
        shard = table[2 * e]
        oy, ox = (y + 4 - shard // 16) % 4, (x + 4 - (shard // 4) % 4) % 4
        oz, oc = (zl + 2 - (shard // 2) % 2) % 2, (core + 2 - shard % 2) % 2
        return position[index(oy, ox, oz, oc)]

    def attend(b):
        attention_block(b, place, q, kv, ctx, lse_own)
        for d in range(1, 4):
            lse_copy(d, b).start()

    stages = ((finish, 6), (forward, 4), (project, 2), (attend, 0))

    def step(i, state):
        for work, lag in stages:
            b = i - lag

            @pl.when(jnp.logical_and(b >= 0, b < NB))
            def _():
                work(b)

        return state

    lax.fori_loop(0, NB + 6, step, 0)

    def drain(ref, sem):
        pltpu.make_async_copy(ref, ref, sem).wait()

    drain(want.at[pl.ds(0, SHARDS - 1)], req_send)
    drain(stage.at[pl.ds(0, SHARDS - 1)], arr_send)
    drain(kv.at[0, 0:6], z_send)
    drain(kv.at[0, 0:6], a_send)
    drain(kv.at[0, 0:36], one_send)
    for group in (0, 1):
        drain(kv.at[0:2, 0:36], two_send.at[group])
        drain(kv.at[0:2, 0:48], c_send.at[group])
    for d in range(3):
        drain(lse_own, lse_send.at[d])
    for way in range(2):
        drain(opp.at[way], opp_send.at[way])
        drain(sendb.at[way], sum_send.at[way])


def whole(table, position, encodings, decoder_states, wq, wk, wv, wo):
    vmem = pl.BlockSpec(memory_space=pltpu.VMEM)
    hbm = pl.BlockSpec(memory_space=pl.ANY)
    dma = pltpu.SemaphoreType.DMA
    return pl.pallas_call(
        kernel,
        out_shape=jax.ShapeDtypeStruct((SEQ_LEN, 256), BF16),
        in_specs=[pl.BlockSpec(memory_space=pltpu.SMEM)] * 2 + [hbm] * 6,
        out_specs=vmem,
        scratch_shapes=[
            pltpu.VMEM((SHARDS, NTOK_PART, D), BF16),
            pltpu.VMEM((SEQ_LEN + SPAN_LEN, D), BF16),
            pltpu.VMEM((SHARDS, 1, 128), jnp.int32),
            pltpu.VMEM((SHARDS, 1, 128), jnp.int32),
            pltpu.SMEM((SHARDS, 1, 128), jnp.int32),
            pltpu.VMEM((SHARDS, NTOK_PART, D), BF16),
            pltpu.VMEM((SHARDS, NTOK_PART, D), BF16),
            pltpu.VMEM((4, 4, 2, 4, 4, 32, 256), BF16),
            pltpu.VMEM((SEQ_LEN, D), BF16),
            pltpu.VMEM((8, D), F32),
            pltpu.VMEM((8, SHARDS, NTOK_PART, GROUP), BF16),
            pltpu.VMEM((NB, BLK, D), BF16),
            pltpu.VMEM((NB, HEADS, BLK), F32),
            pltpu.VMEM((3, NB, HEADS, BLK), F32),
            pltpu.VMEM((2, NB, BLK // 2, 256), BF16),
            pltpu.VMEM((2, NB, BLK // 2, 256), BF16),
            pltpu.VMEM((2, NB, BLK, 256), F32),
            pltpu.VMEM((NB, BLK, 256), F32),
            pltpu.VMEM((2, NB, BLK, 256), BF16),
            pltpu.VMEM((2, NB, BLK, 256), BF16),
            dma((10,)), dma, dma, dma, dma((SHARDS,)),
            dma, dma((3,)), dma, dma((3,)), dma, dma((18,)), dma((2,)), dma((36,)), dma((2,)), dma((12,)),
            dma((3,)), dma((3, NB)), dma((2,)), dma((2, NB)), dma((2,)), dma((2, NB)),
        ],
        compiler_params=pltpu.CompilerParams(
            collective_id=1, has_side_effects=True, vmem_limit_bytes=63 << 20
        ),
        cost_estimate=pl.CostEstimate(
            flops=90_000_000_000, bytes_accessed=16 << 20, transcendentals=1 << 21
        ),
        name="whole",
    )(table, position, encodings, decoder_states, wq, wk, wv, wo)


def body(
    decoder_states, encodings, neighbor_table, query_weight, key_weight, value_weight, out_weight
):
    codes = [((o[0] * 4 + o[1]) * 2 + o[2]) * 2 + o[3] for o in OFFSETS]
    position = jnp.array([codes.index(code) for code in range(SHARDS)], jnp.int32)

    sliced = (2, 4, 4, 32, 256)
    return whole(
        neighbor_table.reshape(-1), position, encodings, decoder_states,
        query_weight.reshape(sliced), key_weight.reshape(sliced), value_weight.reshape(sliced),
        out_weight.reshape(2, 4, 32, D),
    )


def solution(mesh):
    return jax.shard_map(
        body,
        mesh=mesh,
        in_specs=(
            P("span", None),
            P("span", "head", None),
            P("span", None, None),
            P(None, "head"),
            P(None, "head"),
            P(None, "head"),
            P("head", None),
        ),
        out_specs=P("span", "head"),
        check_vma=False,
    )
```

```python
import functools

import jax
import jax.numpy as jnp
from jax import lax
from jax.experimental import pallas as pl
from jax.experimental.pallas import tpu as pltpu
from jax.sharding import PartitionSpec as P

HEAD_DIM = 64
SPAN_LEN = 64
SEQ_LEN = 2048
D = 1024
HEADS = 16
SPANS = 32
SHARDS = 64
NTOK_PART = 32
GROUP = 256
BLK = 128
NB = SEQ_LEN // BLK
QT = 256
F32 = jnp.float32
BF16 = jnp.bfloat16
MESH = pl.DeviceIdType.MESH


def links(o):
    ways = ((0, 0), (1, 0), (1, 1), (0, 1))
    return [*ways[o[1]], *ways[o[0]], o[2]]


def balanced(offsets):
    left, done, order = list(offsets), [0] * 5, []
    while left:

        def cost(o):
            after = [a + b for a, b in zip(done, links(o))]
            mean = sum(after) / 5
            return sum((v - mean) ** 2 for v in after) - sum(links(o))

        best = min(left, key=cost)
        left.remove(best)
        order.append(best)
        done = [a + b for a, b in zip(done, links(best))]
    return order


ALL = [(oy, ox, oz, oc) for oy in range(4) for ox in range(4) for oz in range(2) for oc in range(2)]
OFFSETS = ALL[:1] + balanced(ALL[1:])


def head_mask(rows, cols):
    r = lax.broadcasted_iota(jnp.int32, (rows, cols), 0) // HEAD_DIM
    c = lax.broadcasted_iota(jnp.int32, (rows, cols), 1) // HEAD_DIM
    return r == c


def attention_block(b, place, q, kv, ctx, lse_own):
    mask = head_mask(GROUP, GROUP)
    ones = jnp.where(mask, 1.0, 0.0).astype(BF16)
    zero = jnp.zeros((GROUP, GROUP), BF16)
    lane = lax.broadcasted_iota(jnp.int32, (SPAN_LEN, 128), 1)
    low = lane < HEAD_DIM
    stats = []
    for sp in range(BLK // SPAN_LEN):
        j = b * (BLK // SPAN_LEN) + sp
        first = place(2 * j)
        second = place(2 * j + 1)
        rows = pl.ds(pl.multiple_of(j * SPAN_LEN, SPAN_LEN), SPAN_LEN)
        lses = jnp.zeros((SPAN_LEN, 128), F32)
        for g in range(D // GROUP):
            cols = slice(g * GROUP, (g + 1) * GROUP)
            k4 = jnp.concatenate([kv[g, first], kv[g, second]], axis=0)
            v4 = jnp.concatenate([kv[4 + g, first], kv[4 + g, second]], axis=0)
            kbd = jnp.where(mask, jnp.concatenate([k4] * 4, axis=0), zero)
            vbd = jnp.where(mask, jnp.concatenate([v4] * 4, axis=0), zero)
            s = lax.dot_general(
                q[rows, cols], kbd, (((1,), (1,)), ((), ())), preferred_element_type=F32
            ) * (HEAD_DIM ** -0.5)
            tops = []
            for half in range(2):
                part = s[:, half * 128 : (half + 1) * 128]
                m0 = jnp.max(jnp.where(low, part, -jnp.inf), axis=1, keepdims=True)
                m1 = jnp.max(jnp.where(low, -jnp.inf, part), axis=1, keepdims=True)
                tops.append(jnp.where(low, m0, m1))
            top = jnp.concatenate(tops, axis=1)
            p = jnp.exp(s - top).astype(BF16)
            total = jnp.dot(p, ones, preferred_element_type=F32)
            c = jnp.dot(p, vbd, preferred_element_type=F32)
            ctx[b, sp * SPAN_LEN : (sp + 1) * SPAN_LEN, cols] = (c / total).astype(BF16)
            lse = top + jnp.log(total)
            for n in range(4):
                lses = jnp.where(lane == g * 4 + n, lse[:, n * 64 : n * 64 + 1], lses)
        stats.append(lses)
    lse_own[b] = jnp.concatenate(stats, axis=0).T[:HEADS]


def kernel(
    table, position, enc_hbm, dec_hbm, wq, wk, wv, wo, out,
    enc, dec, req, want, want_s, stage, arr, w, q, carry, kv,
    ctx, lse_own, lse_in, opp, opp_in, side, own, sendb, sum_in,
    load_sem, req_send, req_recv, arr_send, arr_recv,
    z_send, z_recv, a_send, a_recv, one_send, one_recv, two_send, two_recv, c_send, c_recv,
    lse_send, lse_recv, opp_send, opp_recv, sum_send, sum_recv,
):
    h = lax.axis_index("head")
    s = lax.axis_index("span")
    core = s % 2
    zl = (s // 2) % 2
    x = (s // 4) % 4
    y = s // 16
    peers = [(h + d) % 4 for d in range(4)]
    toward = (peers[1], peers[3])

    def index(yy, xx, zz, cc):
        return ((yy * 4 + xx) * 2 + zz) * 2 + cc

    def target(o):
        return index((y + o[0]) % 4, (x + o[1]) % 4, (zl + o[2]) % 2, (core + o[3]) % 2)

    def send(src, dst, send_sem, recv_sem, to):
        return pltpu.make_async_remote_copy(
            src_ref=src, dst_ref=dst, send_sem=send_sem, recv_sem=recv_sem,
            device_id=to, device_id_type=MESH,
        )

    loads = [
        pltpu.make_async_copy(src, w.at[h, i], load_sem.at[i])
        for i, src in ((0, wk), (1, wq), (2, wv))
    ] + [
        pltpu.make_async_copy(
            wo.at[:, :, :, k * 256 : (k + 1) * 256],
            w.at[h, 3, k // 2, 2 * (k % 2) : 2 * (k % 2) + 2],
            load_sem.at[3 + k],
        )
        for k in range(4)
    ]
    enc_load = pltpu.make_async_copy(enc_hbm, enc, load_sem.at[7])
    dec_load = pltpu.make_async_copy(dec_hbm, dec.at[pl.ds(0, SEQ_LEN)], load_sem.at[8])
    for load in loads:
        load.start()
    enc_load.start()
    dec_load.start()

    barrier = pltpu.get_barrier_semaphore()
    for o in OFFSETS[1:]:
        pl.semaphore_signal(barrier, inc=1, device_id={"span": target(o)}, device_id_type=MESH)
    for d in range(1, 4):
        pl.semaphore_signal(barrier, inc=1, device_id={"head": peers[d]}, device_id_type=MESH)
    shard_row = lax.broadcasted_iota(jnp.int32, (SHARDS, 128), 0)
    slots = jnp.zeros((SHARDS, 128), jnp.int32)
    for e in range(SHARDS):
        slots = jnp.where(shard_row == table[2 * e], table[2 * e + 1], slots)
    req[...] = slots.reshape(SHARDS, 1, 128)
    want[s] = req[s]
    dec[SEQ_LEN:] = jnp.zeros((SPAN_LEN, D), BF16)
    pl.semaphore_wait(barrier, SHARDS - 1 + 3)

    for o in OFFSETS[1:]:
        t = target(o)
        send(req.at[t], want.at[s], req_send, req_recv, {"span": t}).start()

    def z_copy(d):
        piece = w.at[h, :, core, y, x, pl.ds(pl.multiple_of(zl * 16, 16), 16), :]
        return send(piece, piece, z_send, z_recv.at[d - 1], {"head": peers[d]})

    def a_copy(d):
        piece = w.at[peers[d], :, core, y, x, pl.ds(pl.multiple_of(zl * 16, 16), 16), :]
        to = {"span": index(y, x, 1 - zl, core)}
        return send(piece, piece, a_send, a_recv.at[d - 1], to)

    def one_copy(half, e, d):
        piece = w.at[peers[d], 2 * half : 2 * half + 2, core, y, x]
        to = index(y, (x + e) % 4, zl, core) if half == 0 else index((y + e) % 4, x, zl, core)
        n = (half * 3 + e - 1) * 3 + d - 1
        return send(piece, piece, one_send, one_recv.at[n], {"span": to})

    def two_copy(group, half, e, d):
        if half == 0:
            piece = w.at[peers[d], group, core, y]
            to = index((y + e) % 4, x, zl, core)
        else:
            piece = w.at[peers[d], 2 + group, core, :, x]
            to = index(y, (x + e) % 4, zl, core)
        n = ((group * 2 + half) * 3 + e - 1) * 3 + d - 1
        return send(piece, piece, two_send.at[group], two_recv.at[n], {"span": to})

    def c_copy(group, half, d):
        piece = w.at[peers[d], 2 * half + group, core]
        n = (group * 2 + half) * 3 + d - 1
        to = {"span": index(y, x, zl, 1 - core)}
        return send(piece, piece, c_send.at[group], c_recv.at[n], to)

    ring = [(half, e, d) for e in (1, 2, 3) for d in (1, 2, 3) for half in (0, 1)]
    swap = [(half, d) for d in (1, 2, 3) for half in (0, 1)]
    def arr_copy(i):
        to = {"span": target(OFFSETS[i])}
        return send(stage.at[i], arr.at[i], arr_send, arr_recv.at[i], to)

    def issue(lo, hi):
        for i in range(lo, hi):
            stage[i] = enc[want_s[target(OFFSETS[i]), 0, 0]]
            if i > 1:
                arr_copy(i - 1).start()

    for load in loads:
        load.wait()
    for d in (1, 2, 3):
        z_copy(d).start()
    everyone = pltpu.make_async_copy(
        want.at[pl.ds(0, SHARDS - 1)], want.at[pl.ds(0, SHARDS - 1)], req_recv
    )
    everyone.wait()
    to_scalar = pltpu.make_async_copy(want, want_s, load_sem.at[9])
    to_scalar.start()
    enc_load.wait()
    to_scalar.wait()
    issue(1, 5)
    for d in (1, 2, 3):
        z_copy(d).wait_recv()
    for d in (1, 2, 3):
        a_copy(d).start()
    issue(5, 9)
    for d in (1, 2, 3):
        a_copy(d).wait_recv()
    for r in ring:
        one_copy(*r).start()
    issue(9, 13)
    for r in ring:
        one_copy(*r).wait_recv()
    for r in ring:
        two_copy(0, *r).start()
    issue(13, 21)
    for r in ring:
        two_copy(0, *r).wait_recv()
    for r in swap:
        c_copy(0, *r).start()
    issue(21, 37)
    for r in ring:
        two_copy(1, *r).start()
    issue(37, SHARDS)
    arr[0] = enc[want_s[s, 0, 0]]
    arr_copy(SHARDS - 1).start()
    for r in swap:
        c_copy(0, *r).wait_recv()

    def weight(group, i):
        return w[group, i].reshape(D, GROUP)

    def project_chunk(k, state):
        for i in range(8):
            n = 8 * k + i

            @pl.when(n > 0)
            def _():
                send(stage.at[n], arr.at[n], arr_send, arr_recv.at[n], {"span": s}).wait_recv()

        tokens = arr[pl.ds(8 * k, 8)].reshape(8 * NTOK_PART, D)

        def columns(n, inner):
            part = jnp.dot(tokens, weight(n % 4, 2 * (n // 4)), preferred_element_type=F32)
            kv[n, pl.ds(8 * k, 8)] = part.astype(BF16).reshape(8, NTOK_PART, GROUP)
            return inner

        return lax.fori_loop(0, 8, columns, state)

    lax.fori_loop(0, 4, project_chunk, 0)
    for r in ring:
        two_copy(1, *r).wait_recv()
    for r in swap:
        c_copy(1, *r).start()
    lax.fori_loop(4, 6, project_chunk, 0)
    dec_load.wait()
    for r in swap:
        c_copy(1, *r).wait_recv()

    for g in range(4):
        head_rows = jnp.dot(dec[48:64], weight(g, 1), preferred_element_type=F32)
        carry[:, g * GROUP : (g + 1) * GROUP] = head_rows[8:16]

    first_row = lax.broadcasted_iota(jnp.int32, (QT, GROUP), 0) == 0

    def query_tile(t, state):
        source = dec[pl.ds(pl.multiple_of(t * QT + 64, 64), QT)]
        for g in range(4):
            cols = slice(g * GROUP, (g + 1) * GROUP)
            tile = jnp.dot(source, weight(g, 1), preferred_element_type=F32)
            before = carry[7:8, cols]
            moved = jnp.where(first_row, before, pltpu.roll(tile, 1, 0))
            q[pl.ds(pl.multiple_of(t * QT, QT), QT), cols] = moved.astype(BF16)
            carry[:, cols] = tile[QT - 8 :]
        return state

    lax.fori_loop(0, SEQ_LEN // QT, query_tile, 0)

    lax.fori_loop(6, SHARDS // 8, project_chunk, 0)

    def lse_copy(d, b):
        return send(
            lse_own.at[b], lse_in.at[d - 1, b], lse_send.at[d - 1], lse_recv.at[d - 1, b],
            {"head": peers[d]},
        )

    def opp_copy(way, b):
        return send(
            opp.at[way, b], opp_in.at[way, b], opp_send.at[way], opp_recv.at[way, b],
            {"head": toward[way]},
        )

    def sum_copy(way, b):
        return send(
            sendb.at[way, b], sum_in.at[way, b], sum_send.at[way], sum_recv.at[way, b],
            {"head": toward[way]},
        )

    row = lax.broadcasted_iota(jnp.int32, (2 * HEADS, D), 0) % HEADS
    col = lax.broadcasted_iota(jnp.int32, (2 * HEADS, D), 1) // HEAD_DIM
    expand = jnp.where(row == col, 1.0, 0.0).astype(BF16)

    def finish(b):
        for way in range(2):
            sum_copy(way, b).wait_recv()
        total = own[b] + (sum_in[0, b].astype(F32) + sum_in[1, b].astype(F32))
        own[b] = total

        @pl.when(b == 0)
        def _():
            last = lax.broadcasted_iota(jnp.int32, (SPAN_LEN, 256), 0) == SPAN_LEN - 1
            out[:SPAN_LEN] = jnp.where(last, total[0:1], 0.0).astype(BF16)

        @pl.when(b > 0)
        def _():
            last = lax.broadcasted_iota(jnp.int32, (BLK, 256), 0) == BLK - 1
            moved = jnp.where(last, total[0:1], pltpu.roll(own[b - 1], BLK - 1, 0))
            out[pl.ds(pl.multiple_of((b - 1) * BLK + SPAN_LEN, SPAN_LEN), BLK)] = moved.astype(BF16)

        @pl.when(b == NB - 1)
        def _():
            out[SEQ_LEN - SPAN_LEN :] = pltpu.roll(total, BLK - 1, 0)[:SPAN_LEN].astype(BF16)

    def forward(b):
        half = BLK // 2
        for way in range(2):
            opp_copy(way, b).wait_recv()
            part = opp_in[way, b].astype(F32)
            if way == 0:
                upper, lower = side[way, b, :half] + part, side[way, b, half:]
            else:
                upper, lower = side[way, b, :half], side[way, b, half:] + part
            sendb[way, b, :half] = upper.astype(BF16)
            sendb[way, b, half:] = lower.astype(BF16)
            sum_copy(way, b).start()

    def project(b):
        for d in range(1, 4):
            lse_copy(d, b).wait_recv()
        mine = lse_own[b]
        others = [lse_in[d, b] for d in range(3)]
        top = jnp.maximum(jnp.maximum(mine, others[0]), jnp.maximum(others[1], others[2]))
        part = jnp.exp(mine - top)
        total = part
        for other in others:
            total = total + jnp.exp(other - top)
        share = part / total
        high = share.astype(BF16).astype(F32)
        both = jnp.concatenate([high, share - high], axis=0).T.astype(BF16)
        wide = jnp.dot(both, expand, preferred_element_type=F32)
        scaled = (ctx[b].astype(F32) * wide).astype(BF16)

        def columns(k):
            total = None
            for g in range(4):
                block = w[g, 3, k // 2, pl.ds(2 * (k % 2), 2)].reshape(GROUP, GROUP)
                part = jnp.dot(
                    scaled[:, g * GROUP : (g + 1) * GROUP], block, preferred_element_type=F32
                )
                total = part if total is None else total + part
            return total

        away = columns(peers[2]).astype(BF16)
        for way in range(2):
            opp[way, b] = away[way * (BLK // 2) : (way + 1) * (BLK // 2)]
        side[0, b] = columns(peers[1])
        for way in range(2):
            opp_copy(way, b).start()
        side[1, b] = columns(peers[3])
        own[b] = columns(h)

    def place(e):
        shard = table[2 * e]
        oy, ox = (y + 4 - shard // 16) % 4, (x + 4 - (shard // 4) % 4) % 4
        oz, oc = (zl + 2 - (shard // 2) % 2) % 2, (core + 2 - shard % 2) % 2
        return position[index(oy, ox, oz, oc)]

    def attend(b):
        attention_block(b, place, q, kv, ctx, lse_own)
        for d in range(1, 4):
            lse_copy(d, b).start()

    stages = ((finish, 8), (forward, 5), (project, 2), (attend, 0))

    def step(i, state):
        for work, lag in stages:
            b = i - lag

            @pl.when(jnp.logical_and(b >= 0, b < NB))
            def _():
                work(b)

        return state

    lax.fori_loop(0, NB + 8, step, 0)

    def drain(ref, sem):
        pltpu.make_async_copy(ref, ref, sem).wait()

    drain(want.at[pl.ds(0, SHARDS - 1)], req_send)
    drain(stage.at[pl.ds(0, SHARDS - 1)], arr_send)
    drain(kv.at[0, 0:6], z_send)
    drain(kv.at[0, 0:6], a_send)
    drain(kv.at[0, 0:36], one_send)
    for group in (0, 1):
        drain(kv.at[0:2, 0:36], two_send.at[group])
        drain(kv.at[0:2, 0:48], c_send.at[group])
    for d in range(3):
        drain(lse_own, lse_send.at[d])
    for way in range(2):
        drain(opp.at[way], opp_send.at[way])
        drain(sendb.at[way], sum_send.at[way])


def whole(table, position, encodings, decoder_states, wq, wk, wv, wo):
    vmem = pl.BlockSpec(memory_space=pltpu.VMEM)
    hbm = pl.BlockSpec(memory_space=pl.ANY)
    dma = pltpu.SemaphoreType.DMA
    return pl.pallas_call(
        kernel,
        out_shape=jax.ShapeDtypeStruct((SEQ_LEN, 256), BF16),
        in_specs=[pl.BlockSpec(memory_space=pltpu.SMEM)] * 2 + [hbm] * 6,
        out_specs=vmem,
        scratch_shapes=[
            pltpu.VMEM((SHARDS, NTOK_PART, D), BF16),
            pltpu.VMEM((SEQ_LEN + SPAN_LEN, D), BF16),
            pltpu.VMEM((SHARDS, 1, 128), jnp.int32),
            pltpu.VMEM((SHARDS, 1, 128), jnp.int32),
            pltpu.SMEM((SHARDS, 1, 128), jnp.int32),
            pltpu.VMEM((SHARDS, NTOK_PART, D), BF16),
            pltpu.VMEM((SHARDS, NTOK_PART, D), BF16),
            pltpu.VMEM((4, 4, 2, 4, 4, 32, 256), BF16),
            pltpu.VMEM((SEQ_LEN, D), BF16),
            pltpu.VMEM((8, D), F32),
            pltpu.VMEM((8, SHARDS, NTOK_PART, GROUP), BF16),
            pltpu.VMEM((NB, BLK, D), BF16),
            pltpu.VMEM((NB, HEADS, BLK), F32),
            pltpu.VMEM((3, NB, HEADS, BLK), F32),
            pltpu.VMEM((2, NB, BLK // 2, 256), BF16),
            pltpu.VMEM((2, NB, BLK // 2, 256), BF16),
            pltpu.VMEM((2, NB, BLK, 256), F32),
            pltpu.VMEM((NB, BLK, 256), F32),
            pltpu.VMEM((2, NB, BLK, 256), BF16),
            pltpu.VMEM((2, NB, BLK, 256), BF16),
            dma((10,)), dma, dma, dma, dma((SHARDS,)),
            dma, dma((3,)), dma, dma((3,)), dma, dma((18,)), dma((2,)), dma((36,)), dma((2,)), dma((12,)),
            dma((3,)), dma((3, NB)), dma((2,)), dma((2, NB)), dma((2,)), dma((2, NB)),
        ],
        compiler_params=pltpu.CompilerParams(
            collective_id=1, has_side_effects=True, vmem_limit_bytes=63 << 20
        ),
        cost_estimate=pl.CostEstimate(
            flops=90_000_000_000, bytes_accessed=16 << 20, transcendentals=1 << 21
        ),
        name="whole",
    )(table, position, encodings, decoder_states, wq, wk, wv, wo)


def body(
    decoder_states, encodings, neighbor_table, query_weight, key_weight, value_weight, out_weight
):
    codes = [((o[0] * 4 + o[1]) * 2 + o[2]) * 2 + o[3] for o in OFFSETS]
    position = jnp.array([codes.index(code) for code in range(SHARDS)], jnp.int32)

    sliced = (2, 4, 4, 32, 256)
    return whole(
        neighbor_table.reshape(-1), position, encodings, decoder_states,
        query_weight.reshape(sliced), key_weight.reshape(sliced), value_weight.reshape(sliced),
        out_weight.reshape(2, 4, 32, D),
    )


def solution(mesh):
    return jax.shard_map(
        body,
        mesh=mesh,
        in_specs=(
            P("span", None),
            P("span", "head", None),
            P("span", None, None),
            P(None, "head"),
            P(None, "head"),
            P(None, "head"),
            P("head", None),
        ),
        out_specs=P("span", "head"),
        check_vma=False,
    )
```
